32 devices in a mesh: space: 32 (over z, y, x, core), mem: 1.
Axes of the slice: x: 2, y: 2, z: 4, core: 2. Of those that a mesh axis runs over, the one named last changes fastest.
Arguments:
- members: bfloat16 [128, 768, 2, 384], P(('space', 'mem')), may hold values from -6 to 6
- state: float32 [768, 2, 384], P('space'), may hold values from -6 to 6
- cotangent: float32 [768, 2, 384], P('space'), may hold values from -6 to 6
- conv_in: float32 [3, 3, 128, 2], replicated, may hold values from -1.5 to 1.5
- conv_out: float32 [3, 3, 2, 128], replicated, may hold values from -0.1875 to 0.1875
- bias: float32 [128], replicated, may hold values from -3 to 3
Outputs:
- increment: float32 [768, 2, 384], P('space')
- response: float32 [768, 2, 384], P('space')
The draws below stay inside these ranges and needn't reach their ends.
All inputs are finite; a program needn't handle non-finite values.
Results may differ from the reference program's by a relative error of at most 0.0045.
Values may be sent and summed in bfloat16 or wider, within the bound.
A program may use at most 64 MiB of HBM per device.

```python
import jax
import jax.numpy as jnp
from jax import lax

LAT = 384
HID = 128
VARS = 2
HALF = 16
LON = 768
MEMBERS = 128


def strengthened(drawn, own_key, source, target, shards_of, factor):
    owner, partner = [(jnp.arange(drawn.shape[axis_at]) // (drawn.shape[axis_at] // shards_of)).reshape([-1 if axis == axis_at else 1 for axis in range(drawn.ndim)]) for axis_at in (source, target)]
    chosen = jax.random.permutation(own_key, shards_of)[partner]
    strong = (owner == chosen) | (owner == (partner + shards_of // 2) % shards_of)
    return jnp.where(strong, factor * drawn, drawn)


def block_scale(rng, shape, shards, low, largest):
    level = 1.0
    for dim, parts in shards:
        steps = jax.random.uniform(jax.random.fold_in(jax.random.fold_in(rng, 6), dim), (parts,), jnp.float32, low / len(shards), largest / len(shards))
        level = level * jnp.repeat(jnp.exp(steps), shape[dim] // parts).reshape((-1,) + (1,) * (len(shape) - 1 - dim))
    return level


def centred(rng, shape, scale, limit, shards=(), kind=jnp.bfloat16):
    result = scale * jax.random.normal(rng, shape, jnp.float32)
    if shards:
        result = result * block_scale(rng, shape, shards, -0.22, 0.18)
    return jnp.clip(result, -limit, limit).astype(kind)


def gaussian_with(stream_key, shape, scale, reach, pieces, heavy, dtype=jnp.bfloat16):
    drawn = scale * jax.random.normal(stream_key, shape, jnp.float32)
    if pieces:
        drawn = drawn * block_scale(stream_key, shape, pieces, -0.22, 0.18)
    return jnp.clip(strengthened(drawn, jax.random.fold_in(stream_key, 3), *heavy), -reach, reach).astype(dtype)


def setup_inputs(seed: int = 0) -> dict:
    splits = jax.random.split(jax.random.key(seed), 7)
    return {
        "members": gaussian_with(splits[0], (MEMBERS, LON, VARS, LAT), 1.0, 6.0, ((0, 32),), (0, 1, 32, 2.75)),
        "state": centred(splits[1], (LON, VARS, LAT), 1.0, 6.0, ((0, 32),), jnp.float32),
        "cotangent": centred(splits[2], (LON, VARS, LAT), 1.0, 6.0, ((0, 32),), jnp.float32),
        "conv_in": centred(splits[3], (3, 3, HID, VARS), (9 * VARS) ** -0.5, 1.5, (), jnp.float32),
        "conv_out": centred(splits[4], (3, 3, VARS, HID), (9 * HID) ** -0.5, 0.1875, (), jnp.float32),
        "bias": centred(splits[5], (HID,), 0.5, 3.0, (), jnp.float32),
    }


def wrap_lon(field):
    return jnp.concatenate([field[-1:], field, field[:1]], axis=0)


def convolve(field, weight):
    padded = jnp.pad(wrap_lon(field), ((0, 0), (0, 0), (1, 1)))
    row_count = field.shape[0]
    lat_count = field.shape[2]
    summed = jnp.zeros((row_count, weight.shape[2], lat_count), jnp.float32)
    for step_lon in range(3):
        for step_lat in range(3):
            window = padded[step_lon:step_lon + row_count, :, step_lat:step_lat + lat_count]
            summed = summed + jnp.einsum("oc,xcy->xoy", weight[step_lon, step_lat], window, precision=lax.Precision.HIGHEST)
    return summed


def flipped(weight):
    return jnp.transpose(weight[::-1, ::-1], (0, 1, 3, 2))


def band_matrix(count, wrap):
    row_index = jnp.arange(count)[:, None]
    col_index = jnp.arange(count)[None, :]
    distance = jnp.abs(row_index - col_index)
    if wrap:
        distance = jnp.minimum(distance, count - distance)
    ratio = distance.astype(jnp.float32) / (HALF + 1.0)
    return jnp.where(distance <= HALF, 1.0 - ratio * ratio, 0.0).astype(jnp.bfloat16)


def reference(members, state, cotangent, conv_in, conv_out, bias):
    activity = jnp.tanh(convolve(state, conv_in) + bias[None, :, None])
    slopes = 1.0 - activity * activity
    backward = slopes * convolve(cotangent, flipped(conv_out))
    gradient = (cotangent + convolve(backward, flipped(conv_in))).astype(jnp.bfloat16)
    lat_loc = band_matrix(LAT, False).astype(jnp.float32)
    lon_loc = band_matrix(LON, True).astype(jnp.float32)
    grad_wide = gradient.astype(jnp.float32)

    def member_step(carry, member):
        member_wide = member.astype(jnp.float32)
        product = (member_wide * grad_wide).astype(jnp.bfloat16).astype(jnp.float32)
        banded = jnp.einsum("xcy,yz->xcz", product, lat_loc, precision=lax.Precision.HIGHEST).astype(jnp.bfloat16).astype(jnp.float32)
        spread = jnp.einsum("zx,xcy->zcy", lon_loc, banded, precision=lax.Precision.HIGHEST)
        return carry + member_wide * spread, None

    start_sum = jnp.zeros(state.shape, jnp.float32)
    summed, unused = lax.scan(member_step, start_sum, members)
    increment = summed / (MEMBERS - 1.0)
    tangent_hidden = slopes * convolve(increment, conv_in)
    response = increment + convolve(tangent_hidden, conv_out)
    return increment, response
```

```python
import functools

import jax
import jax.numpy as jnp
from jax import lax
from jax.experimental import pallas as pl
from jax.experimental.pallas import tpu as pltpu
from jax.sharding import PartitionSpec as P

HALF = 16


def flip(index, stride):
    return index + stride * (1 - 2 * lax.rem(index // stride, 2))


def flip_all(index, mask):
    stride = 1
    while stride <= mask:
        if mask & stride:
            index = flip(index, stride)
        stride *= 2
    return index


def stages_of(count):
    held = [0]
    steps = []
    stride = count // 2
    while stride >= 8:
        steps.append([(stride, list(held))])
        held = held + [m ^ stride for m in held]
        stride //= 2
    half = max(1, len(held) // 2)
    first, second = held[:half], held[half:]
    steps.append([(2, first), (4, second)])
    first = first + [m ^ 2 for m in first]
    second = second + [m ^ 4 for m in second]
    steps.append([(4, first), (2, second)])
    return steps


def greet(me, count, extra=()):
    barrier = pltpu.get_barrier_semaphore()
    friends = list(extra)
    stride = 1
    while stride < count:
        friends.append(flip(me, stride))
        stride *= 2
    for friend in friends:
        pl.semaphore_signal(
            barrier, inc=1, device_id={"space": friend}, device_id_type=pl.DeviceIdType.MESH
        )
    pl.semaphore_wait(barrier, len(friends))


def gather_kernel(count, block_ref, whole_ref, send_sem, recv_sem):
    me = lax.axis_index("space")
    greet(me, count)

    def remote(mask, stride):
        owner = flip_all(me, mask)
        source = block_ref if mask == 0 else whole_ref.at[owner]
        slot = mask ^ stride
        return pltpu.make_async_remote_copy(
            src_ref=source,
            dst_ref=whole_ref.at[owner],
            send_sem=send_sem.at[slot],
            recv_sem=recv_sem.at[slot],
            device_id={"space": flip(me, stride)},
            device_id_type=pl.DeviceIdType.MESH,
        )

    started = []
    pair = []
    for step in stages_of(count):
        now = []
        for position in range(max(len(masks) for stride, masks in step)):
            for stride, masks in step:
                if position < len(masks):
                    copy = remote(masks[position], stride)
                    copy.start()
                    now.append((copy, masks[position] ^ stride))
        if not pair:
            copy = remote(0, 1)
            copy.start()
            pair.append(copy)
            whole_ref[me] = block_ref[...]
        for copy, mask in now:
            copy.wait_recv()
            other = remote(mask, 1)
            other.start()
            pair.append(other)
            started.append(copy)
    for copy in started:
        copy.wait_send()
    for copy in pair:
        copy.wait()


def gather(block):
    count = lax.axis_size("space")
    return pl.pallas_call(
        functools.partial(gather_kernel, count),
        out_shape=jax.ShapeDtypeStruct((count,) + block.shape, block.dtype),
        in_specs=[pl.BlockSpec(memory_space=pltpu.VMEM)],
        out_specs=pl.BlockSpec(memory_space=pltpu.VMEM),
        scratch_shapes=[
            pltpu.SemaphoreType.DMA((count,)),
            pltpu.SemaphoreType.DMA((count,)),
        ],
        compiler_params=pltpu.CompilerParams(collective_id=0, has_side_effects=True),
        name="gather",
    )(block)


def scatter_kernel(
    count, rim, part_ref, sum_ref, left_ref, right_ref,
    out_buf, in_buf, edge_buf, send_sem, recv_sem, edge_send, edge_recv,
):
    me = lax.axis_index("space")
    before, after = lax.rem(me + count - 1, count), lax.rem(me + 1, count)
    greet(me, count, (before, after))
    arrived = {mask: [] for mask in range(count)}

    def value(mask):
        total = part_ref[flip_all(me, mask)]
        for slot in arrived[mask]:
            total = total + in_buf[slot].astype(jnp.float32)
        return total

    sent = []
    for step in [[(1, list(range(0, count, 2)))]] + stages_of(count)[::-1]:
        now = []
        for position in range(max(len(masks) for stride, masks in step)):
            for stride, masks in step:
                if position < len(masks):
                    slot = masks[position] ^ stride
                    out_buf[slot] = value(slot).astype(out_buf.dtype)
                    copy = pltpu.make_async_remote_copy(
                        src_ref=out_buf.at[slot],
                        dst_ref=in_buf.at[slot],
                        send_sem=send_sem.at[slot],
                        recv_sem=recv_sem.at[slot],
                        device_id={"space": flip(me, stride)},
                        device_id_type=pl.DeviceIdType.MESH,
                    )
                    copy.start()
                    now.append((copy, masks[position], slot))
        for copy, mask, slot in now:
            copy.wait_recv()
            arrived[mask].append(slot)
            sent.append(copy)
    total = value(0)
    sum_ref[...] = total
    edge_buf[0] = total[:rim]
    edge_buf[1] = total[total.shape[0] - rim :]
    edges = [
        pltpu.make_async_remote_copy(
            src_ref=edge_buf.at[side],
            dst_ref=target,
            send_sem=edge_send.at[side],
            recv_sem=edge_recv.at[side],
            device_id={"space": friend},
            device_id_type=pl.DeviceIdType.MESH,
        )
        for side, target, friend in ((0, right_ref, before), (1, left_ref, after))
    ]
    for copy in edges:
        copy.start()
    for copy in sent:
        copy.wait_send()
    for copy in edges:
        copy.wait()


def scatter(parts, rim):
    count, rows, lat_count = parts.shape
    return pl.pallas_call(
        functools.partial(scatter_kernel, count, rim),
        out_shape=(
            jax.ShapeDtypeStruct((rows, lat_count), jnp.float32),
            jax.ShapeDtypeStruct((rim, lat_count), jnp.float32),
            jax.ShapeDtypeStruct((rim, lat_count), jnp.float32),
        ),
        in_specs=[pl.BlockSpec(memory_space=pltpu.VMEM)],
        out_specs=(pl.BlockSpec(memory_space=pltpu.VMEM),) * 3,
        scratch_shapes=[
            pltpu.VMEM((count, rows, lat_count), jnp.bfloat16),
            pltpu.VMEM((count, rows, lat_count), jnp.bfloat16),
            pltpu.VMEM((2, rim, lat_count), jnp.float32),
            pltpu.SemaphoreType.DMA((count,)),
            pltpu.SemaphoreType.DMA((count,)),
            pltpu.SemaphoreType.DMA((2,)),
            pltpu.SemaphoreType.DMA((2,)),
        ],
        compiler_params=pltpu.CompilerParams(collective_id=1, has_side_effects=True),
        name="scatter",
    )(parts)


def padded_2(cells, axis, width):
    count = lax.axis_size(axis)
    head = cells[:width]
    tail = cells[cells.shape[0] - width :]
    return jnp.concatenate(
        [
            lax.ppermute(tail, axis, [(i, (i + 1) % count) for i in range(count)]),
            cells,
            lax.ppermute(head, axis, [((i + 1) % count, i) for i in range(count)]),
        ],
        axis=0,
    )


def convolve(padded, weight):
    row_count = padded.shape[0] - 2
    lat_count = padded.shape[2]
    out_count = weight.shape[2]
    in_count = weight.shape[3]
    padded = padded.astype(jnp.bfloat16)
    weight = weight.astype(jnp.bfloat16)
    if out_count <= in_count:
        flattened = weight.reshape(9 * out_count, in_count)
        product = jnp.einsum(
            "kc,xcy->xky", flattened, padded, preferred_element_type=jnp.float32
        )
        product = jnp.pad(product, ((0, 0), (0, 0), (1, 1)))
        summed = jnp.zeros((row_count, out_count, lat_count), jnp.float32)
        for step_lon in range(3):
            for step_lat in range(3):
                tap_index = step_lon * 3 + step_lat
                summed = (
                    summed
                    + product[
                        step_lon : step_lon + row_count,
                        tap_index * out_count : (tap_index + 1) * out_count,
                        step_lat : step_lat + lat_count,
                    ]
                )
        return summed
    lat_padded = jnp.pad(padded, ((0, 0), (0, 0), (1, 1)))
    stacked = jnp.concatenate(
        [
            lat_padded[step_lon : step_lon + row_count, :, step_lat : step_lat + lat_count]
            for step_lon in range(3)
            for step_lat in range(3)
        ],
        axis=1,
    )
    flattened = jnp.transpose(weight, (2, 0, 1, 3)).reshape(out_count, 9 * in_count)
    return jnp.einsum("ok,xky->xoy", flattened, stacked, preferred_element_type=jnp.float32)


def split(values):
    high = lax.reduce_precision(values, 8, 7)
    return high.astype(jnp.bfloat16), (values - high).astype(jnp.bfloat16)


def convolve_fine(padded, weight):
    out_count, in_count = weight.shape[2:]
    upper, lower = split(padded)
    weight_upper, weight_lower = split(weight)
    if out_count <= in_count:
        both = jnp.concatenate([upper, lower], axis=1)
        stacked = jnp.concatenate([weight_upper, weight_lower], axis=2)
        stacked = jnp.concatenate([stacked, stacked], axis=3)
        result = convolve(both, stacked)
        return result[:, :out_count] + result[:, out_count:]
    return convolve(
        jnp.concatenate([upper, lower, upper], axis=1),
        jnp.concatenate([weight_upper, weight_upper, weight_lower], axis=3),
    )


def flipped(weight):
    return jnp.transpose(weight[::-1, ::-1], (0, 1, 3, 2))


def band_matrix(count, wrap):
    row_index = jnp.arange(count)[:, None]
    col_index = jnp.arange(count)[None, :]
    distance = jnp.abs(row_index - col_index)
    if wrap:
        distance = jnp.minimum(distance, count - distance)
    ratio = distance.astype(jnp.float32) / (HALF + 1.0)
    return jnp.where(distance <= HALF, 1.0 - ratio * ratio, 0.0).astype(jnp.bfloat16)


def per_device(members, state, cotangent, conv_in, conv_out, bias):
    row_count, var_count, lat_count = state.shape
    count = lax.axis_size("space")
    direct = count >= 8 and count & (count - 1) == 0
    rim_width = 2
    joined = jnp.concatenate([state, cotangent], axis=1)
    padded = padded_2(joined, "space", rim_width)
    state_pad = padded[:, :var_count]
    cot_pad = padded[:, var_count:]
    activity = jnp.tanh(convolve_fine(state_pad, conv_in) + bias[None, :, None])
    slopes = 1.0 - activity * activity
    backward = slopes * convolve_fine(cot_pad, flipped(conv_out))
    gradient = cotangent + convolve_fine(backward, flipped(conv_in))
    gradient = gradient.astype(jnp.bfloat16)
    if direct:
        flat = gradient.reshape(row_count * var_count, lat_count)
        whole = gather(flat).reshape(count * row_count, var_count, lat_count)
    else:
        whole = lax.all_gather(gradient, "space", axis=0, tiled=True)
    lat_loc = band_matrix(lat_count, False)
    product = (members.astype(jnp.float32) * whole.astype(jnp.float32)[None]).astype(jnp.bfloat16)
    banded = jnp.einsum(
        "mxcy,yz->mxcz", product, lat_loc, preferred_element_type=jnp.float32
    ).astype(jnp.bfloat16)
    lon_loc = band_matrix(banded.shape[1], True)
    spread = jnp.einsum("zx,mxcy->mzcy", lon_loc, banded, preferred_element_type=jnp.float32)
    contrib = jnp.sum(members.astype(jnp.float32) * spread, axis=0)
    member_count = members.shape[0] * lax.axis_size("space") * lax.axis_size("mem")
    if direct:
        own, left, right = scatter(
            contrib.reshape(count, row_count * var_count, lat_count), rim_width * var_count
        )
        total = jnp.concatenate([left, own, right], axis=0)
        total = total.reshape(row_count + 2 * rim_width, var_count, lat_count)
        if lax.axis_size("mem") > 1:
            total = lax.psum(total, "mem")
        incr_pad = total / (member_count - 1.0)
        increment = incr_pad[rim_width : rim_width + row_count]
    else:
        member_sum = lax.psum(contrib, "mem")
        block_sum = lax.psum_scatter(member_sum, "space", scatter_dimension=0, tiled=True)
        increment = block_sum / (member_count - 1.0)
        incr_pad = padded_2(increment, "space", rim_width)
    tangent_hidden = slopes * convolve(incr_pad, conv_in)
    response = increment + convolve(tangent_hidden, conv_out)
    return (increment, response)


def solution(mesh):
    in_specs = (
        P(("space", "mem"), None, None, None),
        P("space", None, None),
        P("space", None, None),
        P(),
        P(),
        P(),
    )
    out_specs = (P("space", None, None), P("space", None, None))
    return jax.shard_map(
        per_device, mesh=mesh, in_specs=in_specs, out_specs=out_specs, check_vma=False
    )
```

```python
import functools

import jax
import jax.numpy as jnp
from jax import lax
from jax.experimental import pallas as pl
from jax.experimental.pallas import tpu as pltpu
from jax.sharding import PartitionSpec as P

HALF = 16


def flip(index, stride):
    return index + stride * (1 - 2 * lax.rem(index // stride, 2))


def flip_all(index, mask):
    stride = 1
    while stride <= mask:
        if mask & stride:
            index = flip(index, stride)
        stride *= 2
    return index


def stages_of(count):
    held = [0]
    steps = []
    stride = count // 2
    while stride >= 8:
        steps.append([(stride, list(held))])
        held = held + [m ^ stride for m in held]
        stride //= 2
    half = max(1, len(held) // 2)
    first, second = held[:half], held[half:]
    steps.append([(2, first), (4, second)])
    first = first + [m ^ 2 for m in first]
    second = second + [m ^ 4 for m in second]
    steps.append([(4, first), (2, second)])
    return steps


def greet(me, count, extra=()):
    barrier = pltpu.get_barrier_semaphore()
    friends = list(extra)
    stride = 1
    while stride < count:
        friends.append(flip(me, stride))
        stride *= 2
    for friend in friends:
        pl.semaphore_signal(
            barrier, inc=1, device_id={"space": friend}, device_id_type=pl.DeviceIdType.MESH
        )
    pl.semaphore_wait(barrier, len(friends))


def gather_kernel(count, block_ref, whole_ref, send_sem, recv_sem):
    me = lax.axis_index("space")
    greet(me, count)

    def remote(mask, stride):
        owner = flip_all(me, mask)
        source = block_ref if mask == 0 else whole_ref.at[owner]
        slot = mask ^ stride
        return pltpu.make_async_remote_copy(
            src_ref=source,
            dst_ref=whole_ref.at[owner],
            send_sem=send_sem.at[slot],
            recv_sem=recv_sem.at[slot],
            device_id={"space": flip(me, stride)},
            device_id_type=pl.DeviceIdType.MESH,
        )

    started = []
    pair = []
    for step in stages_of(count):
        now = []
        for position in range(max(len(masks) for stride, masks in step)):
            for stride, masks in step:
                if position < len(masks):
                    copy = remote(masks[position], stride)
                    copy.start()
                    now.append((copy, masks[position] ^ stride))
        if not pair:
            copy = remote(0, 1)
            copy.start()
            pair.append(copy)
            whole_ref[me] = block_ref[...]
        for copy, mask in now:
            copy.wait_recv()
            other = remote(mask, 1)
            other.start()
            pair.append(other)
            started.append(copy)
    for copy in started:
        copy.wait_send()
    for copy in pair:
        copy.wait()


def gather(block):
    count = lax.axis_size("space")
    return pl.pallas_call(
        functools.partial(gather_kernel, count),
        out_shape=jax.ShapeDtypeStruct((count,) + block.shape, block.dtype),
        in_specs=[pl.BlockSpec(memory_space=pltpu.VMEM)],
        out_specs=pl.BlockSpec(memory_space=pltpu.VMEM),
        scratch_shapes=[
            pltpu.SemaphoreType.DMA((count,)),
            pltpu.SemaphoreType.DMA((count,)),
        ],
        compiler_params=pltpu.CompilerParams(collective_id=0, has_side_effects=True),
        name="gather",
    )(block)


def scatter_kernel(
    count, rim, part_ref, sum_ref, left_ref, right_ref,
    out_buf, in_buf, edge_buf, send_sem, recv_sem, edge_send, edge_recv,
):
    me = lax.axis_index("space")
    before, after = lax.rem(me + count - 1, count), lax.rem(me + 1, count)
    greet(me, count, (before, after))
    arrived = {mask: [] for mask in range(count)}

    def value(mask):
        total = part_ref[flip_all(me, mask)]
        for slot in arrived[mask]:
            total = total + in_buf[slot].astype(jnp.float32)
        return total

    sent = []
    for step in [[(1, list(range(0, count, 2)))]] + stages_of(count)[::-1]:
        now = []
        for position in range(max(len(masks) for stride, masks in step)):
            for stride, masks in step:
                if position < len(masks):
                    slot = masks[position] ^ stride
                    out_buf[slot] = value(slot).astype(out_buf.dtype)
                    copy = pltpu.make_async_remote_copy(
                        src_ref=out_buf.at[slot],
                        dst_ref=in_buf.at[slot],
                        send_sem=send_sem.at[slot],
                        recv_sem=recv_sem.at[slot],
                        device_id={"space": flip(me, stride)},
                        device_id_type=pl.DeviceIdType.MESH,
                    )
                    copy.start()
                    now.append((copy, masks[position], slot))
        for copy, mask, slot in now:
            copy.wait_recv()
            arrived[mask].append(slot)
            sent.append(copy)
    total = value(0)
    sum_ref[...] = total
    edge_buf[0] = total[:rim]
    edge_buf[1] = total[total.shape[0] - rim :]
    edges = [
        pltpu.make_async_remote_copy(
            src_ref=edge_buf.at[side],
            dst_ref=target,
            send_sem=edge_send.at[side],
            recv_sem=edge_recv.at[side],
            device_id={"space": friend},
            device_id_type=pl.DeviceIdType.MESH,
        )
        for side, target, friend in ((0, right_ref, before), (1, left_ref, after))
    ]
    for copy in edges:
        copy.start()
    for copy in sent:
        copy.wait_send()
    for copy in edges:
        copy.wait()


def scatter(parts, rim):
    count, rows, lat_count = parts.shape
    return pl.pallas_call(
        functools.partial(scatter_kernel, count, rim),
        out_shape=(
            jax.ShapeDtypeStruct((rows, lat_count), jnp.float32),
            jax.ShapeDtypeStruct((rim, lat_count), jnp.float32),
            jax.ShapeDtypeStruct((rim, lat_count), jnp.float32),
        ),
        in_specs=[pl.BlockSpec(memory_space=pltpu.VMEM)],
        out_specs=(pl.BlockSpec(memory_space=pltpu.VMEM),) * 3,
        scratch_shapes=[
            pltpu.VMEM((count, rows, lat_count), jnp.bfloat16),
            pltpu.VMEM((count, rows, lat_count), jnp.bfloat16),
            pltpu.VMEM((2, rim, lat_count), jnp.float32),
            pltpu.SemaphoreType.DMA((count,)),
            pltpu.SemaphoreType.DMA((count,)),
            pltpu.SemaphoreType.DMA((2,)),
            pltpu.SemaphoreType.DMA((2,)),
        ],
        compiler_params=pltpu.CompilerParams(collective_id=1, has_side_effects=True),
        name="scatter",
    )(parts)


def covariance_kernel(members_ref, whole_ref, lat_ref, lon_ref, sum_ref, banded_ref):
    lat_count = lat_ref.shape[0]

    @pl.when(pl.program_id(0) == 0)
    def _():
        sum_ref[...] = jnp.zeros_like(sum_ref)

    for start in range(0, whole_ref.shape[1], lat_count):
        columns = slice(start, start + lat_count)
        product = members_ref[0, :, columns].astype(jnp.float32) * whole_ref[:, columns].astype(
            jnp.float32
        )
        banded_ref[:, columns] = jnp.dot(
            product.astype(jnp.bfloat16), lat_ref[...], preferred_element_type=jnp.float32
        ).astype(jnp.bfloat16)
    for start in range(0, whole_ref.shape[1], lat_count):
        columns = slice(start, start + lat_count)
        spread = jnp.dot(
            lon_ref[...], banded_ref[:, columns], preferred_element_type=jnp.float32
        )
        sum_ref[:, columns] += members_ref[0, :, columns].astype(jnp.float32) * spread


def covariance(members, whole, lat_loc, lon_loc):
    count, lon_count, width = members.shape
    return pl.pallas_call(
        covariance_kernel,
        grid=(count,),
        out_shape=jax.ShapeDtypeStruct((lon_count, width), jnp.float32),
        in_specs=[
            pl.BlockSpec((1, lon_count, width), lambda m: (m, 0, 0)),
            pl.BlockSpec(whole.shape, lambda m: (0, 0)),
            pl.BlockSpec(lat_loc.shape, lambda m: (0, 0)),
            pl.BlockSpec(lon_loc.shape, lambda m: (0, 0)),
        ],
        out_specs=pl.BlockSpec((lon_count, width), lambda m: (0, 0)),
        scratch_shapes=[pltpu.VMEM((lon_count, width), jnp.bfloat16)],
        name="covariance",
    )(members, whole, lat_loc, lon_loc)


def padded_2(cells, axis, width):
    count = lax.axis_size(axis)
    head = cells[:width]
    tail = cells[cells.shape[0] - width :]
    return jnp.concatenate(
        [
            lax.ppermute(tail, axis, [(i, (i + 1) % count) for i in range(count)]),
            cells,
            lax.ppermute(head, axis, [((i + 1) % count, i) for i in range(count)]),
        ],
        axis=0,
    )


def convolve(padded, weight, precision=None):
    row_count = padded.shape[0] - 2
    lat_count = padded.shape[2]
    out_count = weight.shape[2]
    in_count = weight.shape[3]
    if precision is None:
        padded = padded.astype(jnp.bfloat16)
        weight = weight.astype(jnp.bfloat16)
    if out_count <= in_count:
        flattened = weight.reshape(9 * out_count, in_count)
        product = jnp.einsum(
            "kc,xcy->xky", flattened, padded, preferred_element_type=jnp.float32
        )
        product = jnp.pad(product, ((0, 0), (0, 0), (1, 1)))
        summed = jnp.zeros((row_count, out_count, lat_count), jnp.float32)
        for step_lon in range(3):
            for step_lat in range(3):
                tap_index = step_lon * 3 + step_lat
                summed = (
                    summed
                    + product[
                        step_lon : step_lon + row_count,
                        tap_index * out_count : (tap_index + 1) * out_count,
                        step_lat : step_lat + lat_count,
                    ]
                )
        return summed
    lat_padded = jnp.pad(padded, ((0, 0), (0, 0), (1, 1)))
    stacked = jnp.concatenate(
        [
            lat_padded[step_lon : step_lon + row_count, :, step_lat : step_lat + lat_count]
            for step_lon in range(3)
            for step_lat in range(3)
        ],
        axis=1,
    )
    flattened = jnp.transpose(weight, (2, 0, 1, 3)).reshape(out_count, 9 * in_count)
    return jnp.einsum(
        "ok,xky->xoy", flattened, stacked, precision=precision, preferred_element_type=jnp.float32
    )


def split(values):
    high = lax.reduce_precision(values, 8, 7)
    return high.astype(jnp.bfloat16), (values - high).astype(jnp.bfloat16)


def convolve_fine(padded, weight):
    out_count, in_count = weight.shape[2:]
    upper, lower = split(padded)
    weight_upper, weight_lower = split(weight)
    if out_count <= in_count:
        both = jnp.concatenate([upper, lower], axis=1)
        stacked = jnp.concatenate([weight_upper, weight_lower], axis=2)
        stacked = jnp.concatenate([stacked, stacked], axis=3)
        result = convolve(both, stacked)
        return result[:, :out_count] + result[:, out_count:]
    return convolve(padded, weight, lax.Precision.HIGH)


def flipped(weight):
    return jnp.transpose(weight[::-1, ::-1], (0, 1, 3, 2))


def band_matrix(count, wrap):
    row_index = jnp.arange(count)[:, None]
    col_index = jnp.arange(count)[None, :]
    distance = jnp.abs(row_index - col_index)
    if wrap:
        distance = jnp.minimum(distance, count - distance)
    ratio = distance.astype(jnp.float32) / (HALF + 1.0)
    return jnp.where(distance <= HALF, 1.0 - ratio * ratio, 0.0).astype(jnp.bfloat16)


def per_device(members, state, cotangent, conv_in, conv_out, bias):
    row_count, var_count, lat_count = state.shape
    count = lax.axis_size("space")
    direct = count >= 8 and count & (count - 1) == 0
    rim_width = 2
    joined = jnp.concatenate([state, cotangent], axis=1)
    padded = padded_2(joined, "space", rim_width)
    state_pad = padded[:, :var_count]
    cot_pad = padded[:, var_count:]
    activity = jnp.tanh(convolve_fine(state_pad, conv_in) + bias[None, :, None])
    slopes = 1.0 - activity * activity
    backward = slopes * convolve_fine(cot_pad, flipped(conv_out))
    gradient = cotangent + convolve_fine(backward, flipped(conv_in))
    gradient = gradient.astype(jnp.bfloat16)
    width = var_count * lat_count
    gradient = gradient.reshape(row_count, width)
    if direct:
        whole = gather(gradient).reshape(count * row_count, width)
    else:
        whole = lax.all_gather(gradient, "space", axis=0, tiled=True)
    merged = members.reshape(members.shape[0], members.shape[1], width)
    lat_loc = band_matrix(lat_count, False)
    lon_loc = band_matrix(merged.shape[1], True)
    contrib = covariance(merged, whole, lat_loc, lon_loc)
    member_count = members.shape[0] * lax.axis_size("space") * lax.axis_size("mem")
    if direct:
        own, left, right = scatter(
            contrib.reshape(count, row_count, width), rim_width
        )
        total = jnp.concatenate([left, own, right], axis=0)
        total = total.reshape(row_count + 2 * rim_width, var_count, lat_count)
        if lax.axis_size("mem") > 1:
            total = lax.psum(total, "mem")
        incr_pad = total / (member_count - 1.0)
        increment = incr_pad[rim_width : rim_width + row_count]
    else:
        member_sum = lax.psum(contrib, "mem")
        block_sum = lax.psum_scatter(member_sum, "space", scatter_dimension=0, tiled=True)
        increment = block_sum.reshape(state.shape) / (member_count - 1.0)
        incr_pad = padded_2(increment, "space", rim_width)
    tangent_hidden = slopes * convolve(incr_pad, conv_in)
    response = increment + convolve(tangent_hidden, conv_out)
    return (increment, response)


def solution(mesh):
    in_specs = (
        P(("space", "mem"), None, None, None),
        P("space", None, None),
        P("space", None, None),
        P(),
        P(),
        P(),
    )
    out_specs = (P("space", None, None), P("space", None, None))
    return jax.shard_map(
        per_device, mesh=mesh, in_specs=in_specs, out_specs=out_specs, check_vma=False
    )
```
